32 devices in a mesh: member: 2 (over x), row: 16 (over z, y, core).
Axes of the slice: x: 2, y: 2, z: 4, core: 2. Of those that a mesh axis runs over, the one named last changes fastest.
Arguments:
- field: float32 [8, 6, 2048, 2048], P('member', None, 'row'), parts along dimension 0, as said below
- host: float32 [128, 2, 8, 6, 128], P('row', None, 'member'), parts along dimension 2, may hold values from -0.12 to 0.12
- weights: float32 [8, 4], replicated, may hold values from 0.1 to 1
- cut_x: int32 [6], replicated, may hold values from 16 to 63
- cut_y: int32 [6], replicated, may hold values from 16 to 63
- table_index: int32 [6], replicated, may hold values from 0 to 7
Outputs:
- nudged: float32 [8, 6, 2048, 2048], P('member', None, 'row'), parts along dimension 0
The draws below stay inside these ranges and needn't reach their ends.
There are 2 independent parts, one for each index of `member`. The reference program is written for one: setup_inputs(seed, part) draws one part's arguments, and reference() takes and returns one part's arrays. A program takes and returns all parts, laid end to end along the dimension named above; an argument that names none is the same for every part. Nothing has to cross between parts.
Inputs may be any that keep to these rules, and one draw needn't show every extreme that they name: `field`: real-valued fields with strong large-scale structure.
All inputs are finite; a program needn't handle non-finite values.
Results may differ from the reference program's by a relative error of at most 0.00005.
Values sent between devices are 32-bit elements; how exact they have to be, the bound alone decides.
No kernel may reach another device: no remote copies, remote signals or barrier semaphores. Data moves between devices by JAX's collectives and lax.ppermute only.
A program may use at most 128 MiB of HBM per device.

```python
import math
import jax
import jax.numpy as jnp
from jax import lax

NX = 2048
NY = 2048
VARS = 4
LEVELS = 6
KHALF = 64
TABLE = 8
KBOX = 128


def draw_field(key, part):
    first_key, second_key = jax.random.split(jax.random.fold_in(key, 17), 2)
    signed = jnp.arange(KBOX, dtype=jnp.int32) - KHALF
    phase_x = jnp.mod(jnp.arange(NX, dtype=jnp.int32)[:, None] * signed[None, :], NX).astype(jnp.float32) * (2.0 * math.pi / NX)
    phase_y = jnp.mod(jnp.arange(NY, dtype=jnp.int32)[:, None] * signed[None, :], NY).astype(jnp.float32) * (2.0 * math.pi / NY)
    coeffs = 0.011 * jax.random.normal(second_key, (2, VARS, LEVELS, KBOX, KBOX), jnp.float32)
    noise = 0.5 * jax.random.normal(first_key, (VARS, LEVELS, NX, NY), jnp.float32)
    cos_x = jnp.cos(phase_x)
    sin_x = jnp.sin(phase_x)
    real_part = jnp.einsum('xa,vlab->vlxb', cos_x, coeffs[0]) - jnp.einsum('xa,vlab->vlxb', sin_x, coeffs[1])
    imag_part = jnp.einsum('xa,vlab->vlxb', sin_x, coeffs[0]) + jnp.einsum('xa,vlab->vlxb', cos_x, coeffs[1])
    smooth = jnp.einsum('vlxb,yb->vlxy', real_part, jnp.cos(phase_y)) - jnp.einsum('vlxb,yb->vlxy', imag_part, jnp.sin(phase_y))
    return (smooth + noise).astype(jnp.float32)


def set_ends(drawn, own_key, low, high):
    longest = drawn.shape.index(max(drawn.shape))
    spots = []
    for shift in (0, 1):
        where = [jax.random.randint(jax.random.fold_in(own_key, axis), (), 0, length) for axis, length in enumerate(drawn.shape)]
        where[longest] = (where[longest] + shift) % drawn.shape[longest]
        spots.append(tuple(where))
    return drawn.at[spots[0]].set(low).at[spots[1]].set(high)


def shard_levels(stream_key, shape, pieces, low, high):
    level = 1.0
    for position, blocks in pieces:
        draws = jax.random.uniform(jax.random.fold_in(jax.random.fold_in(stream_key, 6), position), (blocks,), jnp.float32, low / len(pieces), high / len(pieces))
        level = level * jnp.repeat(jnp.exp(draws), shape[position] // blocks).reshape((-1,) + (1,) * (len(shape) - 1 - position))
    return level


def centred(stream_key, extent, spread, limit, cuts=(), kind=jnp.bfloat16):
    values = jax.random.normal(stream_key, extent, jnp.float32) * spread
    if len(cuts) > 0:
        values = shard_levels(stream_key, extent, cuts, -0.22, 0.18) * values
    return jnp.clip(values, min=-limit, max=limit).astype(kind)


def setup_inputs(seed: int = 0, part: int = 0) -> dict:
    keys = jax.random.split(jax.random.key(seed), 7)
    part_splits = jax.random.split(jax.random.fold_in(keys[6], part), 7)
    field = draw_field(jax.random.fold_in(jax.random.fold_in(keys[6], part), 71), part)
    host = centred(part_splits[1], (KBOX, 2, VARS, LEVELS, KBOX), 0.02, 0.12, ((0, 16),), jnp.float32)
    weights = jnp.clip(jnp.exp(jax.random.uniform(keys[2], (TABLE, VARS), jnp.float32, math.log(0.1), math.log(1.0))), 0.1, 1.0)
    cut_x = set_ends(jax.random.randint(keys[3], (LEVELS,), KHALF // 4, KHALF), jax.random.fold_in(keys[3], 1), KHALF // 4, KHALF - 1).astype(jnp.int32)
    cut_y = set_ends(jax.random.randint(keys[4], (LEVELS,), KHALF // 4, KHALF), jax.random.fold_in(keys[4], 1), KHALF // 4, KHALF - 1).astype(jnp.int32)
    table_index = set_ends(jax.random.randint(keys[5], (LEVELS,), 0, TABLE), jax.random.fold_in(keys[5], 1), 0, TABLE - 1).astype(jnp.int32)
    return dict(field=field, host=host, weights=weights, cut_x=cut_x, cut_y=cut_y, table_index=table_index)


def box_wave(index):
    half = index // 2
    return jnp.where(index % 2 == 0, half, jnp.where(index == 1, -KHALF, -half)).astype(jnp.int32)


def reference(field, host, weights, cut_x, cut_y, table_index):
    signed = jnp.arange(KBOX, dtype=jnp.int32) - KHALF
    y_waves = box_wave(jnp.arange(KBOX, dtype=jnp.int32))
    onehot = (table_index[:, None] == jnp.arange(TABLE, dtype=jnp.int32)[None, :]).astype(jnp.float32)
    blend = jnp.dot(onehot, weights, precision=lax.Precision.HIGHEST)
    mask_x = (jnp.abs(signed)[None, :] <= cut_x[:, None]).astype(jnp.float32)
    mask_y = (jnp.abs(y_waves)[None, :] <= cut_y[:, None]).astype(jnp.float32)
    index_x = jnp.mod(signed, NX).astype(jnp.int32)
    index_y = jnp.mod(y_waves, NY).astype(jnp.int32)
    flat = field.reshape(VARS * LEVELS, NX, NY)

    def forward(grid):
        spectrum = jnp.fft.fft2(grid) / (NX * NY)
        boxed = spectrum[index_x[:, None], index_y[None, :]]
        return jnp.stack([jnp.real(boxed), jnp.imag(boxed)], 0).astype(field.dtype)

    boxes = lax.map(forward, flat).reshape(VARS, LEVELS, 2, KBOX, KBOX)
    spectrum = jnp.transpose(boxes, (4, 2, 0, 1, 3))
    scale = blend.T[None, None, :, :, None] * mask_y.T[:, None, None, :, None] * mask_x[None, None, None, :, :]
    delta = scale * (host - spectrum)
    ordered = jnp.transpose(delta, (2, 3, 1, 4, 0)).reshape(VARS * LEVELS, 2, KBOX, KBOX)

    def inverse(pair):
        grid, parts = pair
        boxed = parts[0] + 1j * parts[1]
        whole = jnp.zeros((NX, NY), dtype=boxed.dtype)
        whole = whole.at[index_x[:, None], index_y[None, :]].set(boxed)
        correction = jnp.real(jnp.fft.ifft2(whole)) * (NX * NY)
        return grid + correction.astype(grid.dtype)

    result = lax.map(inverse, (flat, ordered))
    return result.reshape(VARS, LEVELS, NX, NY)
```

```python
import math

import jax
import jax.numpy as jnp
import numpy as np
from jax import lax
from jax.experimental import pallas as pl
from jax.experimental.pallas import tpu as pltpu
from jax.sharding import PartitionSpec as P

BF16 = jnp.bfloat16
F32 = jnp.float32
CHUNKS = 1
GROUP_FORWARD = 4
GROUP_INVERSE = 4
STAGES = 3
AHEAD = 4


def box_wave(index, half_box):
    half = index // 2
    return jnp.where(index % 2 == 0, half, jnp.where(index == 1, -half_box, -half))


def wave_tables(positions, length, waves):
    phase = jnp.mod(positions[:, None] * waves[None, :], length).astype(F32) * (
        2.0 * math.pi / length
    )
    return (jnp.cos(phase), jnp.sin(phase))


def any_cutoff(field, host, weights, cut_x, cut_y, table_index):
    high = lax.Precision.HIGHEST
    row_count = field.shape[2]
    devices = lax.axis_size("row")
    place = lax.axis_index("row")
    nx = row_count * devices
    ny = field.shape[3]
    box = host.shape[4]
    local_rows = place * row_count + lax.iota(jnp.int32, row_count)
    x_waves = lax.iota(jnp.int32, box) - box // 2
    y_waves = box_wave(lax.iota(jnp.int32, box), box // 2)
    owned = box // devices
    cos_y, sin_y = wave_tables(lax.iota(jnp.int32, ny), ny, y_waves)
    table_y = jnp.stack([cos_y, -sin_y], 1) / ny
    cos_x, sin_x = wave_tables(local_rows, nx, x_waves)
    table_x = jnp.stack([jnp.stack([cos_x, -sin_x], 1), jnp.stack([sin_x, cos_x], 1)], 0) / nx
    back_x = jnp.stack([jnp.stack([cos_x.T, sin_x.T], 1), jnp.stack([-sin_x.T, cos_x.T], 1)], 0)
    back_y = jnp.stack([cos_y.T, -sin_y.T], 1)

    def ahead(plane):
        spread = jnp.einsum("lxy,yck->kclx", plane, table_y, precision=high)
        return jnp.einsum("kclx,cxdq->kdlq", spread, table_x, precision=high)

    slots = lax.iota(jnp.int32, devices) ^ place
    partial = jnp.transpose(lax.map(ahead, field), (1, 2, 0, 3, 4))
    partial = partial.reshape(devices, owned, *partial.shape[1:])[slots]
    spectrum = reduce_to_owner(partial[0::2], partial[1::2], devices)
    own_index = place * owned + lax.iota(jnp.int32, owned)
    blend = weights[table_index]
    mask_x = (jnp.abs(x_waves)[None, :] <= cut_x[:, None]).astype(F32)
    mask_y = (jnp.abs(box_wave(own_index, box // 2))[:, None] <= cut_y[None, :]).astype(F32)
    delta = (
        blend.T[None, None, :, :, None]
        * mask_y[:, None, None, :, None]
        * mask_x[None, None, None, :, :]
        * (host - spectrum)
    )
    whole = jnp.stack(gather_from_owners(delta, devices), 1).reshape(devices, *delta.shape)[slots]
    whole = jnp.transpose(whole.reshape(box, *delta.shape[1:]), (2, 0, 1, 3, 4))

    def behind(pair):
        plane, part = pair
        back = jnp.einsum("kclq,cqdx->kdlx", part, back_x, precision=high)
        return plane + jnp.einsum("kclx,kcy->lxy", back, back_y, precision=high)

    return lax.map(behind, (field, whole))


def basis(length, box):
    index = np.arange(box)
    wave = np.where(index == 1, box // 2, index // 2)
    phase = (np.arange(length)[:, None] * wave[None, :]) % length * (2.0 * math.pi / length)
    table = np.where((index % 2 == 0) | (index == 1), np.cos(phase), np.sin(phase))
    high = table.astype(np.float32).astype(BF16)
    low = (table - high.astype(np.float64)).astype(np.float32).astype(BF16)
    return high, low


def split(value):
    high = value.astype(BF16)
    return high, (value - high.astype(F32)).astype(BF16)


def dot(a, b, dims=((1,), (0,))):
    return lax.dot_general(a, b, (dims, ((), ())), preferred_element_type=F32)


def forward(field, table, table_x, place, first, count, devices):
    _, rows, ny = field.shape
    box = table.shape[1] // 2
    owned = box // devices
    group = math.gcd(GROUP_FORWARD, count)
    steps = count // group

    def kernel(
        place_ref, field_ref, far_ref, far_x_ref, slots_ref, held_ref,
        table_ref, table_x_ref, y_ref, arrived, ready,
    ):
        me = place_ref[0]
        tables = (
            pltpu.make_async_copy(far_ref, table_ref, ready.at[0]),
            pltpu.make_async_copy(far_x_ref.at[pl.ds(me * rows, rows)], table_x_ref, ready.at[1]),
        )

        def copy(i):
            return pltpu.make_async_copy(
                field_ref.at[pl.ds(first + i * group, group)],
                held_ref.at[pl.ds(i * group, group)],
                arrived.at[i],
            )

        def along_y(i):
            x = held_ref[pl.ds(i * group, group)].reshape(group * rows, ny)
            high, low = split(x)
            wide = dot(high, table_ref[...])
            y_ref[...] = wide[:, :box] + wide[:, box:] + dot(low, table_ref[:, :box])

        def along_x(i):
            y = y_ref[...]
            y = jnp.concatenate([y[g * rows : (g + 1) * rows].T for g in range(group)], 0)
            high, low = split(y)
            wide = dot(high, table_x_ref[...])
            t = wide[:, :box] + wide[:, box:] + dot(low, table_x_ref[:, :box])
            for owner in range(devices):
                slot = jnp.bitwise_xor(owner, me)
                slot = (slot & 1) * (devices // 2) + (slot >> 1)
                for g in range(group):
                    at = g * box + owner * owned
                    slots_ref[slot, i * group + g] = t[at : at + owned]

        copy(0).start()
        for table_copy in tables:
            table_copy.start()
        for table_copy in tables:
            table_copy.wait()
        for i in range(1, min(AHEAD, steps)):
            copy(i).start()
        copy(0).wait()
        along_y(0)

        @pl.loop(1, steps)
        def _(i):
            @pl.when(i + AHEAD - 1 < steps)
            def _():
                copy(i + AHEAD - 1).start()

            copy(i).wait()
            along_x(i - 1)
            along_y(i)

        along_x(steps - 1)

    slots = jax.ShapeDtypeStruct((devices, count, owned, box), F32)
    vmem = pl.BlockSpec(memory_space=pltpu.VMEM)
    return pl.pallas_call(
        kernel,
        name="forward",
        out_shape=(slots, pltpu.VMEM((count, rows, ny), F32)),
        in_specs=[
            pl.BlockSpec(memory_space=pltpu.SMEM),
            pl.BlockSpec(memory_space=pltpu.HBM),
            pl.BlockSpec(memory_space=pltpu.HBM),
            pl.BlockSpec(memory_space=pltpu.HBM),
        ],
        out_specs=(vmem, vmem),
        scratch_shapes=[
            pltpu.VMEM((ny, 2 * box), BF16),
            pltpu.VMEM((rows, 2 * box), BF16),
            pltpu.VMEM((group * rows, box), F32),
            pltpu.SemaphoreType.DMA((steps,)),
            pltpu.SemaphoreType.DMA((2,)),
        ],
        compiler_params=pltpu.CompilerParams(vmem_limit_bytes=24 << 20),
        cost_estimate=pl.CostEstimate(
            flops=2 * 3 * count * rows * ny * box,
            bytes_accessed=4 * count * rows * ny,
            transcendentals=0,
        ),
    )(place, *(pltpu.with_memory_space_constraint(a, pltpu.HBM) for a in (field, table, table_x)))


def inverse(held, slots, back, table_x, place, first, out, total):
    count, rows, ny = held.shape
    devices, _, owned, box = slots.shape
    group = math.gcd(GROUP_INVERSE, count)
    steps = count // group
    stages = min(STAGES, steps)

    def kernel(place_ref, held_ref, slots_ref, back_ref, table_x_ref, *rest):
        out_ref, coefficients, lines, stage, sent = rest[-5:]
        me = place_ref[0]
        x_table = table_x_ref[pl.ds(me * rows, rows), :]
        x_high = x_table[:, :box]
        x_low = x_table[:, box:]
        last = ((1,), (1,))

        def copy(i):
            slot = i % stages
            return pltpu.make_async_copy(
                stage.at[slot], out_ref.at[pl.ds(first + i * group, group)], sent.at[slot]
            )

        @pl.loop(0, steps)
        def _(i):
            for owner in range(devices):
                slot = jnp.bitwise_xor(owner, me)
                slot = (slot & 1) * (devices // 2) + (slot >> 1)
                for g in range(group):
                    at = g * box + owner * owned
                    coefficients[at : at + owned] = slots_ref[slot, i * group + g]
            d_high, d_low = split(coefficients[...])
            for g in range(group):
                high = d_high[g * box : (g + 1) * box]
                low = d_low[g * box : (g + 1) * box]
                line = dot(x_high, high, last) + dot(x_low, high, last) + dot(x_high, low, last)
                high, low = split(line)
                at = slice(g * rows, (g + 1) * rows)
                lines[i, at, :box] = high
                lines[i, at, box : 2 * box] = low
                lines[i, at, 2 * box :] = high

        @pl.loop(0, steps)
        def _(i):
            change = dot(lines[i], back_ref[...])

            @pl.when(i >= stages)
            def _():
                copy(i - stages).wait()

            stage[i % stages] = held_ref[pl.ds(i * group, group)] + change.reshape(group, rows, ny)
            copy(i).start()

        for i in range(steps - stages, steps):
            copy(i).wait()

    vmem = pl.BlockSpec(memory_space=pltpu.VMEM)
    hbm = pl.BlockSpec(memory_space=pl.ANY)
    in_specs = [pl.BlockSpec(memory_space=pltpu.SMEM), vmem, vmem, vmem, vmem]
    held = pltpu.with_memory_space_constraint(held, pltpu.VMEM)
    args = [place, held, slots, back, table_x]
    alias = {}
    if out is not None:
        in_specs.append(hbm)
        args.append(out)
        alias = {5: 0}
    return pl.pallas_call(
        kernel,
        name="inverse",
        out_shape=jax.ShapeDtypeStruct((total, rows, ny), F32),
        in_specs=in_specs,
        out_specs=hbm,
        scratch_shapes=[
            pltpu.VMEM((group * box, box), F32),
            pltpu.VMEM((steps, group * rows, 3 * box), BF16),
            pltpu.VMEM((stages, group, rows, ny), F32),
            pltpu.SemaphoreType.DMA((stages,)),
        ],
        input_output_aliases=alias,
        compiler_params=pltpu.CompilerParams(vmem_limit_bytes=28 << 20),
        cost_estimate=pl.CostEstimate(
            flops=2 * 3 * count * rows * ny * box,
            bytes_accessed=4 * count * rows * ny,
            transcendentals=0,
        ),
    )(*args)


def exchange(value, bit, devices):
    return lax.ppermute(value, "row", [(i, i ^ bit) for i in range(devices)])


def reduce_to_owner(keep, send, devices):
    total = keep + exchange(send, 1, devices)
    pairs = total.reshape(devices // 4, 2, *total.shape[1:])
    total = pairs[:, 0] + exchange(pairs[:, 1], 2, devices)
    moved = [exchange(total[k], 4 * k, devices) for k in range(1, devices // 4)]
    result = total[0]
    for piece in moved:
        result = result + piece
    return result


def gather_from_owners(own, devices):
    pieces = jnp.stack([own] + [exchange(own, 4 * k, devices) for k in range(1, devices // 4)])
    pieces = jnp.stack([pieces, exchange(pieces, 2, devices)], 1)
    pieces = pieces.reshape(devices // 2, *own.shape)
    return pieces, exchange(pieces, 1, devices)


def host_terms(host, weights, cut_x, cut_y, table_index, place, table, nx, ny):
    owned, _, variables, levels, box = host.shape
    half_box = box // 2
    fields = variables * levels
    signed = np.arange(box)[:, None] - half_box
    target = np.arange(box)[None, :]
    match = (np.abs(signed) == target // 2) & (np.abs(signed) < half_box)
    to_cos = np.where(match & (target % 2 == 0), 1.0, 0.0)
    to_sin = np.where(match & (target % 2 == 1), -np.sign(signed), 0.0)
    fold = jnp.asarray(np.concatenate([to_cos, to_sin], 0).astype(BF16))

    def kernel(
        place_ref, weights_ref, cut_x_ref, cut_y_ref, index_ref, host_ref, fold_ref, table_ref,
        wanted_ref, factor_ref, back_ref, rows_ref,
    ):
        j = lax.broadcasted_iota(jnp.int32, (owned, box), 0)
        a = lax.broadcasted_iota(jnp.int32, (owned, box), 1)
        b = place_ref[0] * owned + j
        even = j % 2 == 0
        wave_x = jnp.where(a == 1, half_box, a >> 1)
        wave_y = jnp.where(b == 1, half_box, b >> 1)
        twice = jnp.where(a == 0, 1.0, 2.0) * jnp.where(b == 0, 1.0, 2.0) / (nx * ny)

        def partner(value):
            return jnp.where(even, jnp.roll(value, -1, 0), jnp.roll(value, 1, 0))

        for v in range(variables):
            for l in range(levels):
                at = v * levels + l
                real = jnp.where(b == 1, 0.0, host_ref[:, 0, v, l, :])
                imag = jnp.where(b == 1, 0.0, host_ref[:, 1, v, l, :])
                real_pair, imag_pair = partner(real), partner(imag)
                rows = slice(at * owned, (at + 1) * owned)
                rows_ref[rows, :box] = jnp.where(even, real + real_pair, imag - imag_pair)
                rows_ref[rows, box:] = jnp.where(even, imag + imag_pair, real_pair - real)
        rest = rows_ref[...]
        folded = jnp.zeros((fields * owned, box), F32)
        for _ in range(3):
            part = rest.astype(BF16)
            rest = rest - part.astype(F32)
            folded = folded + dot(part, fold_ref[...])
        for v in range(variables):
            for l in range(levels):
                at = v * levels + l
                inside = (wave_x <= cut_x_ref[l]) & (wave_y <= cut_y_ref[l])
                scale = jnp.where(inside, weights_ref[v, index_ref[l]], 0.0)
                wanted_ref[at] = scale * folded[at * owned : (at + 1) * owned]
                factor_ref[at] = scale * twice
        back_ref[:box] = table_ref[:, :box].T
        back_ref[box : 2 * box] = back_ref[:box]
        back_ref[2 * box :] = table_ref[:, box:].T

    smem = pl.BlockSpec(memory_space=pltpu.SMEM)
    vmem = pl.BlockSpec(memory_space=pltpu.VMEM)
    flat = jax.ShapeDtypeStruct((fields, owned, box), F32)
    return pl.pallas_call(
        kernel,
        name="host_terms",
        out_shape=(flat, flat, jax.ShapeDtypeStruct((3 * box, ny), BF16)),
        in_specs=[smem, smem, smem, smem, smem, vmem, vmem, vmem],
        out_specs=(vmem, vmem, vmem),
        scratch_shapes=[pltpu.VMEM((fields * owned, 2 * box), F32)],
        compiler_params=pltpu.CompilerParams(vmem_limit_bytes=8 << 20),
    )(place, weights.T, cut_x, cut_y, table_index, host, fold, table)


def all_below(cut_x, cut_y, edge):
    def kernel(cut_x_ref, cut_y_ref, out_ref):
        most = cut_x_ref[0]
        for ref in (cut_x_ref, cut_y_ref):
            for i in range(ref.shape[0]):
                most = jnp.maximum(most, ref[i])
        out_ref[0] = (most < edge).astype(jnp.int32)

    smem = pl.BlockSpec(memory_space=pltpu.SMEM)
    return pl.pallas_call(
        kernel,
        name="all_below",
        out_shape=jax.ShapeDtypeStruct((1,), jnp.int32),
        in_specs=[smem, smem],
        out_specs=smem,
    )(cut_x, cut_y)[0]


def below_edge(field, host, weights, cut_x, cut_y, table_index):
    variables, levels, rows, ny = field.shape
    devices = lax.axis_size("row")
    place = lax.axis_index("row")
    nx = rows * devices
    box = host.shape[4]
    fields = variables * levels
    flat = field.reshape(fields, rows, ny)
    me = place.astype(jnp.int32).reshape(1)
    high, low = basis(ny, box)
    table = jnp.asarray(np.concatenate([high, low], 1))
    if nx == ny:
        table_x = table
    else:
        table_x = jnp.asarray(np.concatenate(basis(nx, box), 1))
    wanted, factor, back = host_terms(host, weights, cut_x, cut_y, table_index, me, table, nx, ny)
    count = fields // CHUNKS
    firsts = [c * count for c in range(CHUNKS)]
    sums = [forward(flat, table, table_x, me, first, count, devices) for first in firsts]
    gathered = []
    for first, (slots, _) in zip(firsts, sums):
        total = reduce_to_owner(slots[: devices // 2], slots[devices // 2 :], devices)
        part = slice(first, first + count)
        gathered.append(
            jnp.concatenate(gather_from_owners(wanted[part] - factor[part] * total, devices), 0)
        )
    out = None
    for first, slots, (_, held) in zip(firsts, gathered, sums):
        out = inverse(held, slots, back, table_x, me, first, out, fields)
    return out.reshape(field.shape)


def shards(field, host, weights, cut_x, cut_y, table_index):
    edge = host.shape[4] // 2
    inside = all_below(cut_x, cut_y, edge)
    args = (field, host, weights, cut_x, cut_y, table_index)
    return lax.switch(inside, (any_cutoff, below_edge), *args)


def solution(mesh):
    return jax.shard_map(
        shards,
        mesh=mesh,
        in_specs=(
            P("member", None, "row", None),
            P("row", None, "member", None, None),
            P(),
            P(),
            P(),
            P(),
        ),
        out_specs=P("member", None, "row", None),
        check_vma=False,
    )
```

```python
import math

import jax
import jax.numpy as jnp
import numpy as np
from jax import lax
from jax.experimental import pallas as pl
from jax.experimental.pallas import tpu as pltpu
from jax.sharding import PartitionSpec as P

BF16 = jnp.bfloat16
F32 = jnp.float32
GROUP_FORWARD = 4
GROUP_INVERSE = 4
STAGES = 3
AHEAD = 3
TILE = 512


def box_wave(index, half_box):
    half = index // 2
    return jnp.where(index % 2 == 0, half, jnp.where(index == 1, -half_box, -half))


def wave_tables(positions, length, waves):
    phase = jnp.mod(positions[:, None] * waves[None, :], length).astype(F32) * (
        2.0 * math.pi / length
    )
    return (jnp.cos(phase), jnp.sin(phase))


def any_cutoff(field, host, weights, cut_x, cut_y, table_index):
    high = lax.Precision.HIGHEST
    row_count = field.shape[2]
    devices = lax.axis_size("row")
    place = lax.axis_index("row")
    nx = row_count * devices
    ny = field.shape[3]
    box = host.shape[4]
    local_rows = place * row_count + lax.iota(jnp.int32, row_count)
    x_waves = lax.iota(jnp.int32, box) - box // 2
    y_waves = box_wave(lax.iota(jnp.int32, box), box // 2)
    owned = box // devices
    cos_y, sin_y = wave_tables(lax.iota(jnp.int32, ny), ny, y_waves)
    table_y = jnp.stack([cos_y, -sin_y], 1) / ny
    cos_x, sin_x = wave_tables(local_rows, nx, x_waves)
    table_x = jnp.stack([jnp.stack([cos_x, -sin_x], 1), jnp.stack([sin_x, cos_x], 1)], 0) / nx
    back_x = jnp.stack([jnp.stack([cos_x.T, sin_x.T], 1), jnp.stack([-sin_x.T, cos_x.T], 1)], 0)
    back_y = jnp.stack([cos_y.T, -sin_y.T], 1)

    def ahead(plane):
        spread = jnp.einsum("lxy,yck->kclx", plane, table_y, precision=high)
        return jnp.einsum("kclx,cxdq->kdlq", spread, table_x, precision=high)

    slots = lax.iota(jnp.int32, devices) ^ place
    partial = jnp.transpose(lax.map(ahead, field), (1, 2, 0, 3, 4))
    partial = partial.reshape(devices, owned, *partial.shape[1:])[slots]
    spectrum = reduce_to_owner(partial[0::2], partial[1::2], devices)
    own_index = place * owned + lax.iota(jnp.int32, owned)
    blend = weights[table_index]
    mask_x = (jnp.abs(x_waves)[None, :] <= cut_x[:, None]).astype(F32)
    mask_y = (jnp.abs(box_wave(own_index, box // 2))[:, None] <= cut_y[None, :]).astype(F32)
    delta = (
        blend.T[None, None, :, :, None]
        * mask_y[:, None, None, :, None]
        * mask_x[None, None, None, :, :]
        * (host - spectrum)
    )
    whole = jnp.stack(gather_from_owners(delta, devices), 1).reshape(devices, *delta.shape)[slots]
    whole = jnp.transpose(whole.reshape(box, *delta.shape[1:]), (2, 0, 1, 3, 4))

    def behind(pair):
        plane, part = pair
        back = jnp.einsum("kclq,cqdx->kdlx", part, back_x, precision=high)
        return plane + jnp.einsum("kclx,kcy->lxy", back, back_y, precision=high)

    return lax.map(behind, (field, whole))


def basis(length, box):
    index = np.arange(box)
    wave = np.where(index == 1, box // 2, index // 2)
    phase = (np.arange(length)[:, None] * wave[None, :]) % length * (2.0 * math.pi / length)
    table = np.where((index % 2 == 0) | (index == 1), np.cos(phase), np.sin(phase))
    high = table.astype(np.float32).astype(BF16)
    low = (table - high.astype(np.float64)).astype(np.float32).astype(BF16)
    return high, low


def split(value):
    high = value.astype(BF16)
    return high, (value - high.astype(F32)).astype(BF16)


def dot(a, b, dims=((1,), (0,))):
    return lax.dot_general(a, b, (dims, ((), ())), preferred_element_type=F32)


def forward(field, table, table_x, place, devices):
    count, rows, ny = field.shape
    box = table.shape[1] // 2
    owned = box // devices
    group = math.gcd(GROUP_FORWARD, count)
    steps = count // group

    def kernel(
        place_ref, field_ref, far_ref, far_x_ref, slots_ref, held_ref,
        table_ref, table_x_ref, y_ref, arrived, ready,
    ):
        me = place_ref[0]
        tables = (
            pltpu.make_async_copy(far_ref, table_ref, ready.at[0]),
            pltpu.make_async_copy(far_x_ref.at[pl.ds(me * rows, rows)], table_x_ref, ready.at[1]),
        )

        def copy(i):
            return pltpu.make_async_copy(
                field_ref.at[pl.ds(i * group, group)],
                held_ref.at[pl.ds(i * group, group)],
                arrived.at[i],
            )

        def along_y(i):
            x = held_ref[pl.ds(i * group, group)].reshape(group * rows, ny)
            high, low = split(x)
            wide = dot(high, table_ref[...])
            y_ref[...] = wide[:, :box] + wide[:, box:] + dot(low, table_ref[:, :box])

        def along_x(i):
            y = y_ref[...]
            y = jnp.concatenate([y[g * rows : (g + 1) * rows].T for g in range(group)], 0)
            high, low = split(y)
            wide = dot(high, table_x_ref[...])
            t = wide[:, :box] + wide[:, box:] + dot(low, table_x_ref[:, :box])
            for owner in range(devices):
                slot = jnp.bitwise_xor(owner, me)
                slot = (slot & 1) * (devices // 2) + (slot >> 1)
                for g in range(group):
                    at = g * box + owner * owned
                    slots_ref[slot, i * group + g] = t[at : at + owned]

        copy(0).start()
        for table_copy in tables:
            table_copy.start()
        for table_copy in tables:
            table_copy.wait()
        for i in range(1, min(AHEAD, steps)):
            copy(i).start()
        copy(0).wait()
        along_y(0)

        @pl.loop(1, steps)
        def _(i):
            @pl.when(i + AHEAD - 1 < steps)
            def _():
                copy(i + AHEAD - 1).start()

            copy(i).wait()
            along_x(i - 1)
            along_y(i)

        along_x(steps - 1)

    slots = jax.ShapeDtypeStruct((devices, count, owned, box), F32)
    vmem = pl.BlockSpec(memory_space=pltpu.VMEM)
    return pl.pallas_call(
        kernel,
        name="forward",
        out_shape=(slots, pltpu.VMEM((count, rows, ny), F32)),
        in_specs=[
            pl.BlockSpec(memory_space=pltpu.SMEM),
            pl.BlockSpec(memory_space=pltpu.HBM),
            pl.BlockSpec(memory_space=pltpu.HBM),
            pl.BlockSpec(memory_space=pltpu.HBM),
        ],
        out_specs=(vmem, vmem),
        scratch_shapes=[
            pltpu.VMEM((ny, 2 * box), BF16),
            pltpu.VMEM((rows, 2 * box), BF16),
            pltpu.VMEM((group * rows, box), F32),
            pltpu.SemaphoreType.DMA((steps,)),
            pltpu.SemaphoreType.DMA((2,)),
        ],
        compiler_params=pltpu.CompilerParams(vmem_limit_bytes=24 << 20),
        cost_estimate=pl.CostEstimate(
            flops=2 * 3 * count * rows * ny * box,
            bytes_accessed=4 * count * rows * ny,
            transcendentals=0,
        ),
    )(place, *(pltpu.with_memory_space_constraint(a, pltpu.HBM) for a in (field, table, table_x)))


def inverse(held, slots, back, x_back, place):
    count, rows, ny = held.shape
    devices, _, owned, box = slots.shape
    group = math.gcd(GROUP_INVERSE, count)
    steps = count // group
    stages = min(STAGES, steps)
    tile = math.gcd(TILE, ny // 2)

    def kernel(
        place_ref, held_ref, slots_ref, back_ref, x_back_ref, out_ref,
        coefficients, lines, stage, sent,
    ):
        me = place_ref[0]

        def copy(i):
            slot = i % stages
            return pltpu.make_async_copy(
                stage.at[slot], out_ref.at[pl.ds(i * group, group)], sent.at[slot]
            )

        def along_x(i):
            for owner in range(devices):
                slot = jnp.bitwise_xor(owner, me)
                slot = (slot & 1) * (devices // 2) + (slot >> 1)
                for g in range(group):
                    at = g * box + owner * owned
                    coefficients[at : at + owned] = slots_ref[slot, i * group + g]
            sorted_rows = [
                coefficients[pl.ds(g * box + r, box // 4, stride=4)]
                for g in range(group)
                for r in range(4)
            ]
            high, low = split(jnp.concatenate(sorted_rows, 0))
            turned = dot(jnp.concatenate([high, low, high], 1), x_back_ref[...])
            high, low = split(turned)
            for g in range(group):
                even = slice(g * box, g * box + box // 2)
                odd = slice(g * box + box // 2, (g + 1) * box)
                at = slice(g * rows, (g + 1) * rows)
                lines[i, at, :box] = jnp.concatenate([high[even], low[even]], 0).T
                lines[i, at, box : 2 * box] = high[g * box : (g + 1) * box].T
                lines[i, at, 2 * box :] = jnp.concatenate([high[odd], low[odd]], 0).T

        def along_y(i):
            slot = i % stages
            mine = pl.ds(i * group, group)
            for n in range(0, ny // 2, tile):
                at = slice(n, n + tile)
                even = dot(lines[i, :, : 2 * box], back_ref[0, :, at]).reshape(group, rows, tile)
                odd = dot(lines[i, :, box:], back_ref[1, :, at]).reshape(group, rows, tile)
                for start, change in ((n, even + odd), (n + ny // 2, even - odd)):
                    at = pl.ds(start, tile)
                    stage[slot, :, :, at] = held_ref[mine, :, at] + change
                    pltpu.make_async_copy(
                        stage.at[slot, :, :, at], out_ref.at[mine, :, at], sent.at[slot]
                    ).start()

        along_x(0)

        @pl.loop(0, steps)
        def _(i):
            @pl.when(i >= stages)
            def _():
                copy(i - stages).wait()

            along_y(i)
            along_x(jnp.minimum(i + 1, steps - 1))

        for i in range(steps - stages, steps):
            copy(i).wait()

    vmem = pl.BlockSpec(memory_space=pltpu.VMEM)
    hbm = pl.BlockSpec(memory_space=pl.ANY)
    in_specs = [pl.BlockSpec(memory_space=pltpu.SMEM), vmem, vmem, vmem, vmem]
    near = [pltpu.with_memory_space_constraint(a, pltpu.VMEM) for a in (held, slots, back, x_back)]
    return pl.pallas_call(
        kernel,
        name="inverse",
        out_shape=jax.ShapeDtypeStruct(held.shape, F32),
        in_specs=in_specs,
        out_specs=hbm,
        scratch_shapes=[
            pltpu.VMEM((group * box, box), F32),
            pltpu.VMEM((steps, group * rows, 3 * box), BF16),
            pltpu.VMEM((stages, group, rows, ny), F32),
            pltpu.SemaphoreType.DMA((stages,)),
        ],
        compiler_params=pltpu.CompilerParams(vmem_limit_bytes=28 << 20),
        cost_estimate=pl.CostEstimate(
            flops=2 * 3 * count * rows * ny * box,
            bytes_accessed=4 * count * rows * ny,
            transcendentals=0,
        ),
    )(place, *near)


def exchange(value, bit, devices):
    return lax.ppermute(value, "row", [(i, i ^ bit) for i in range(devices)])


def reduce_to_owner(keep, send, devices):
    rest = range(1, devices // 4)
    total = keep + exchange(send, 1, devices)
    pairs = total.reshape(devices // 4, 2, *total.shape[1:])
    cut = total.shape[1] * 2 // 3
    here, there = pairs[:, :, :cut], pairs[:, :, cut:]
    one = exchange(here[:, 1], 2, devices)
    others = [exchange(there[k], 4 * k, devices) for k in rest]
    here = here[:, 0] + one
    there = sum(others, there[0])
    others = [exchange(here[k], 4 * k, devices) for k in rest]
    one = exchange(there[1], 2, devices)
    return jnp.concatenate([sum(others, here[0]), there[0] + one], 0)


def gather_from_owners(own, devices):
    rest = range(1, devices // 4)
    cut = own.shape[0] // 2
    here, there = own[:cut], own[cut:]
    one = exchange(there, 2, devices)
    others = [exchange(here, 4 * k, devices) for k in rest]
    there = jnp.stack([there, one])
    here = jnp.stack([here, *others])
    others = [exchange(there, 4 * k, devices) for k in rest]
    one = exchange(here, 2, devices)
    pieces = jnp.concatenate([jnp.stack([here, one], 1), jnp.stack([there, *others])], 2)
    pieces = pieces.reshape(devices // 2, *own.shape)
    return pieces, exchange(pieces, 1, devices)


def prepare(host, weights, cut_x, cut_y, table_index, place, table, table_x, rows, nx, ny):
    owned, _, variables, levels, box = host.shape
    half_box = box // 2
    fields = variables * levels
    signed = np.arange(box)[:, None] - half_box
    target = np.arange(box)[None, :]
    match = (np.abs(signed) == target // 2) & (np.abs(signed) < half_box)
    to_cos = np.where(match & (target % 2 == 0), 1.0, 0.0)
    to_sin = np.where(match & (target % 2 == 1), -np.sign(signed), 0.0)
    fold = jnp.asarray(np.concatenate([to_cos, to_sin], 0).astype(BF16))

    def kernel(
        place_ref, weights_ref, cut_x_ref, cut_y_ref, index_ref, host_ref, fold_ref, table_ref,
        far_x_ref, wanted_ref, factor_ref, back_ref, x_back_ref, rows_ref, table_x_ref, turned_ref, arrived,
    ):
        fetch = pltpu.make_async_copy(
            far_x_ref.at[pl.ds(place_ref[0] * rows, rows)], table_x_ref, arrived.at[0]
        )
        fetch.start()
        j = lax.broadcasted_iota(jnp.int32, (owned, box), 0)
        a = lax.broadcasted_iota(jnp.int32, (owned, box), 1)
        b = place_ref[0] * owned + j
        even = j % 2 == 0
        wave_x = jnp.where(a == 1, half_box, a >> 1)
        wave_y = jnp.where(b == 1, half_box, b >> 1)
        twice = jnp.where(a == 0, 1.0, 2.0) * jnp.where(b == 0, 1.0, 2.0) / (nx * ny)

        def partner(value):
            return jnp.where(even, jnp.roll(value, -1, 0), jnp.roll(value, 1, 0))

        for v in range(variables):
            for l in range(levels):
                at = v * levels + l
                real = jnp.where(b == 1, 0.0, host_ref[:, 0, v, l, :])
                imag = jnp.where(b == 1, 0.0, host_ref[:, 1, v, l, :])
                real_pair, imag_pair = partner(real), partner(imag)
                own = slice(at * owned, (at + 1) * owned)
                rows_ref[own, :box] = jnp.where(even, real + real_pair, imag - imag_pair)
                rows_ref[own, box:] = jnp.where(even, imag + imag_pair, real_pair - real)
        rest = rows_ref[...]
        folded = jnp.zeros((fields * owned, box), F32)
        for _ in range(3):
            part = rest.astype(BF16)
            rest = rest - part.astype(F32)
            folded = folded + dot(part, fold_ref[...])
        for v in range(variables):
            for l in range(levels):
                at = v * levels + l
                inside = (wave_x <= cut_x_ref[l]) & (wave_y <= cut_y_ref[l])
                scale = jnp.where(inside, weights_ref[v, index_ref[l]], 0.0)
                wanted_ref[at] = scale * folded[at * owned : (at + 1) * owned]
                factor_ref[at] = scale * twice
        fetch.wait()
        high = table_x_ref[:, :box].T
        x_back_ref[:box] = high
        x_back_ref[box : 2 * box] = high
        x_back_ref[2 * box :] = table_x_ref[:, box:].T
        quarter, half = box // 4, box // 2
        none = jnp.zeros((half, ny // 2), BF16)
        back_ref[0, 3 * half :] = none
        back_ref[1, :half] = none
        for c in range(0, ny // 2, box):
            at = slice(c, c + box)
            for part in range(2):
                turned_ref[...] = table_ref[at, part * box : (part + 1) * box].astype(F32).T
                rows_of = [turned_ref[pl.ds(r, quarter, stride=4)] for r in range(4)]
                even = jnp.concatenate(rows_of[:2], 0).astype(BF16)
                odd = jnp.concatenate(rows_of[2:], 0).astype(BF16)
                if part == 0:
                    back_ref[0, :half, at] = even
                    back_ref[0, half : 2 * half, at] = even
                    back_ref[1, 2 * half : 3 * half, at] = odd
                    back_ref[1, 3 * half :, at] = odd
                else:
                    back_ref[0, 2 * half : 3 * half, at] = even
                    back_ref[1, half : 2 * half, at] = odd

    smem = pl.BlockSpec(memory_space=pltpu.SMEM)
    vmem = pl.BlockSpec(memory_space=pltpu.VMEM)
    far_x = pltpu.with_memory_space_constraint(table_x, pltpu.HBM)
    flat = jax.ShapeDtypeStruct((fields, owned, box), F32)
    return pl.pallas_call(
        kernel,
        name="prepare",
        out_shape=(flat, flat, pltpu.VMEM((2, 2 * box, ny // 2), BF16), pltpu.VMEM((3 * box, rows), BF16)),
        in_specs=[smem] * 5 + [vmem] * 3 + [pl.BlockSpec(memory_space=pltpu.HBM)],
        out_specs=(vmem, vmem, vmem, vmem),
        scratch_shapes=[
            pltpu.VMEM((fields * owned, 2 * box), F32),
            pltpu.VMEM((rows, 2 * box), BF16),
            pltpu.VMEM((box, box), F32),
            pltpu.SemaphoreType.DMA((1,)),
        ],
        compiler_params=pltpu.CompilerParams(vmem_limit_bytes=8 << 20),
    )(place, weights.T, cut_x, cut_y, table_index, host, fold, table, far_x)


def all_below(cut_x, cut_y, edge):
    def kernel(cut_x_ref, cut_y_ref, out_ref):
        most = cut_x_ref[0]
        for ref in (cut_x_ref, cut_y_ref):
            for i in range(ref.shape[0]):
                most = jnp.maximum(most, ref[i])
        out_ref[0] = (most < edge).astype(jnp.int32)

    smem = pl.BlockSpec(memory_space=pltpu.SMEM)
    return pl.pallas_call(
        kernel,
        name="all_below",
        out_shape=jax.ShapeDtypeStruct((1,), jnp.int32),
        in_specs=[smem, smem],
        out_specs=smem,
        compiler_params=pltpu.CompilerParams(vmem_limit_bytes=1 << 20),
    )(cut_x, cut_y)[0]


def below_edge(field, host, weights, cut_x, cut_y, table_index):
    variables, levels, rows, ny = field.shape
    devices = lax.axis_size("row")
    place = lax.axis_index("row")
    nx = rows * devices
    box = host.shape[4]
    fields = variables * levels
    flat = field.reshape(fields, rows, ny)
    me = place.astype(jnp.int32).reshape(1)
    high, low = basis(ny, box)
    table = jnp.asarray(np.concatenate([high, low], 1))
    if nx == ny:
        table_x = table
    else:
        table_x = jnp.asarray(np.concatenate(basis(nx, box), 1))
    wanted, factor, back, x_back = prepare(
        host, weights, cut_x, cut_y, table_index, me, table, table_x, rows, nx, ny
    )
    slots, held = forward(flat, table, table_x, me, devices)
    total = reduce_to_owner(slots[: devices // 2], slots[devices // 2 :], devices)
    slots = jnp.concatenate(gather_from_owners(wanted - factor * total, devices), 0)
    out = inverse(held, slots, back, x_back, me)
    return out.reshape(field.shape)


def shards(field, host, weights, cut_x, cut_y, table_index):
    edge = host.shape[4] // 2
    inside = all_below(cut_x, cut_y, edge)
    args = (field, host, weights, cut_x, cut_y, table_index)
    branches = (lambda out, *rest: any_cutoff(*rest), lambda out, *rest: out)
    return lax.switch(inside, branches, below_edge(*args), *args)


def solution(mesh):
    return jax.shard_map(
        shards,
        mesh=mesh,
        in_specs=(
            P("member", None, "row", None),
            P("row", None, "member", None, None),
            P(),
            P(),
            P(),
            P(),
        ),
        out_specs=P("member", None, "row", None),
        check_vma=False,
    )
```

```python
import math

import jax
import jax.numpy as jnp
import numpy as np
from jax import lax
from jax.experimental import pallas as pl
from jax.experimental.pallas import tpu as pltpu
from jax.sharding import PartitionSpec as P


BF16 = jnp.bfloat16
F32 = jnp.float32
GROUP_FORWARD = 4
GROUP_INVERSE = 4
STAGES = 3
AHEAD = 3
TILE = 512


def box_wave(index, half_box):
    half = index // 2
    return jnp.where(index % 2 == 0, half, jnp.where(index == 1, -half_box, -half))


def wave_tables(positions, length, waves):
    phase = jnp.mod(positions[:, None] * waves[None, :], length).astype(F32) * (
        2.0 * math.pi / length
    )
    return (jnp.cos(phase), jnp.sin(phase))


def any_cutoff(field, host, weights, cut_x, cut_y, table_index):
    high = lax.Precision.HIGHEST
    row_count = field.shape[2]
    devices = lax.axis_size("row")
    place = lax.axis_index("row")
    nx = row_count * devices
    ny = field.shape[3]
    box = host.shape[4]
    local_rows = place * row_count + lax.iota(jnp.int32, row_count)
    x_waves = lax.iota(jnp.int32, box) - box // 2
    y_waves = box_wave(lax.iota(jnp.int32, box), box // 2)
    owned = box // devices
    cos_y, sin_y = wave_tables(lax.iota(jnp.int32, ny), ny, y_waves)
    table_y = jnp.stack([cos_y, -sin_y], 1) / ny
    cos_x, sin_x = wave_tables(local_rows, nx, x_waves)
    table_x = jnp.stack([jnp.stack([cos_x, -sin_x], 1), jnp.stack([sin_x, cos_x], 1)], 0) / nx
    back_x = jnp.stack([jnp.stack([cos_x.T, sin_x.T], 1), jnp.stack([-sin_x.T, cos_x.T], 1)], 0)
    back_y = jnp.stack([cos_y.T, -sin_y.T], 1)

    def ahead(plane):
        spread = jnp.einsum("lxy,yck->kclx", plane, table_y, precision=high)
        return jnp.einsum("kclx,cxdq->kdlq", spread, table_x, precision=high)

    slots = lax.iota(jnp.int32, devices) ^ place
    partial = jnp.transpose(lax.map(ahead, field), (1, 2, 0, 3, 4))
    partial = partial.reshape(devices, owned, *partial.shape[1:])[slots]
    spectrum = reduce_to_owner(partial[0::2], partial[1::2], devices)
    own_index = place * owned + lax.iota(jnp.int32, owned)
    blend = weights[table_index]
    mask_x = (jnp.abs(x_waves)[None, :] <= cut_x[:, None]).astype(F32)
    mask_y = (jnp.abs(box_wave(own_index, box // 2))[:, None] <= cut_y[None, :]).astype(F32)
    delta = (
        blend.T[None, None, :, :, None]
        * mask_y[:, None, None, :, None]
        * mask_x[None, None, None, :, :]
        * (host - spectrum)
    )
    whole = jnp.stack(gather_from_owners(delta, devices), 1).reshape(devices, *delta.shape)[slots]
    whole = jnp.transpose(whole.reshape(box, *delta.shape[1:]), (2, 0, 1, 3, 4))

    def behind(pair):
        plane, part = pair
        back = jnp.einsum("kclq,cqdx->kdlx", part, back_x, precision=high)
        return plane + jnp.einsum("kclx,kcy->lxy", back, back_y, precision=high)

    return lax.map(behind, (field, whole))


def basis(length, box):
    index = np.arange(box)
    wave = np.where(index == 1, box // 2, index // 2)
    phase = (np.arange(length)[:, None] * wave[None, :]) % length * (2.0 * math.pi / length)
    table = np.where((index % 2 == 0) | (index == 1), np.cos(phase), np.sin(phase))
    high = table.astype(np.float32).astype(BF16)
    low = (table - high.astype(np.float64)).astype(np.float32).astype(BF16)
    return high, low


def split(value):
    high = value.astype(BF16)
    return high, (value - high.astype(F32)).astype(BF16)


def dot(a, b, dims=((1,), (0,))):
    return lax.dot_general(a, b, (dims, ((), ())), preferred_element_type=F32)


def forward(field, table, table_x, place, devices):
    count, rows, ny = field.shape
    box = table.shape[1] // 2
    owned = box // devices
    group = math.gcd(GROUP_FORWARD, count)
    steps = count // group

    def kernel(
        place_ref, field_ref, far_ref, far_x_ref, slots_ref, held_ref,
        table_ref, table_x_ref, y_ref, arrived, ready,
    ):
        me = place_ref[0]
        tables = (
            pltpu.make_async_copy(far_ref, table_ref, ready.at[0]),
            pltpu.make_async_copy(far_x_ref.at[pl.ds(me * rows, rows)], table_x_ref, ready.at[1]),
        )

        def copy(i):
            return pltpu.make_async_copy(
                field_ref.at[pl.ds(i * group, group)],
                held_ref.at[pl.ds(i * group, group)],
                arrived.at[i],
            )

        def along_y(i):
            x = held_ref[pl.ds(i * group, group)].reshape(group * rows, ny)
            high, low = split(x)
            wide = dot(high, table_ref[...])
            y_ref[...] = wide[:, :box] + wide[:, box:] + dot(low, table_ref[:, :box])

        def along_x(i):
            y = y_ref[...]
            y = jnp.concatenate([y[g * rows : (g + 1) * rows].T for g in range(group)], 0)
            high, low = split(y)
            wide = dot(high, table_x_ref[...])
            t = wide[:, :box] + wide[:, box:] + dot(low, table_x_ref[:, :box])
            for owner in range(devices):
                slot = jnp.bitwise_xor(owner, me)
                slot = (slot & 1) * (devices // 2) + (slot >> 1)
                for g in range(group):
                    at = g * box + owner * owned
                    slots_ref[slot, i * group + g] = t[at : at + owned]

        copy(0).start()
        for table_copy in tables:
            table_copy.start()
        for table_copy in tables:
            table_copy.wait()
        for i in range(1, min(AHEAD, steps)):
            copy(i).start()
        copy(0).wait()
        along_y(0)

        @pl.loop(1, steps)
        def _(i):
            @pl.when(i + AHEAD - 1 < steps)
            def _():
                copy(i + AHEAD - 1).start()

            copy(i).wait()
            along_x(i - 1)
            along_y(i)

        along_x(steps - 1)

    slots = jax.ShapeDtypeStruct((devices, count, owned, box), F32)
    vmem = pl.BlockSpec(memory_space=pltpu.VMEM)
    return pl.pallas_call(
        kernel,
        name="forward",
        out_shape=(slots, pltpu.VMEM((count, rows, ny), F32)),
        in_specs=[
            pl.BlockSpec(memory_space=pltpu.SMEM),
            pl.BlockSpec(memory_space=pltpu.HBM),
            pl.BlockSpec(memory_space=pltpu.HBM),
            pl.BlockSpec(memory_space=pltpu.HBM),
        ],
        out_specs=(vmem, vmem),
        scratch_shapes=[
            pltpu.VMEM((ny, 2 * box), BF16),
            pltpu.VMEM((rows, 2 * box), BF16),
            pltpu.VMEM((group * rows, box), F32),
            pltpu.SemaphoreType.DMA((steps,)),
            pltpu.SemaphoreType.DMA((2,)),
        ],
        compiler_params=pltpu.CompilerParams(vmem_limit_bytes=24 << 20),
        cost_estimate=pl.CostEstimate(
            flops=2 * 3 * count * rows * ny * box,
            bytes_accessed=4 * count * rows * ny,
            transcendentals=0,
        ),
    )(place, *(pltpu.with_memory_space_constraint(a, pltpu.HBM) for a in (field, table, table_x)))


def inverse(held, slots, back, x_back, place):
    count, rows, ny = held.shape
    devices, _, owned, box = slots.shape
    group = math.gcd(GROUP_INVERSE, count)
    steps = count // group
    stages = min(STAGES, steps)
    tile = math.gcd(TILE, ny // 2)

    def kernel(
        place_ref, held_ref, slots_ref, back_ref, x_back_ref, out_ref,
        coefficients, lines, stage, sent,
    ):
        me = place_ref[0]

        def copy(i):
            slot = i % stages
            return pltpu.make_async_copy(
                stage.at[slot], out_ref.at[pl.ds(i * group, group)], sent.at[slot]
            )

        def along_x(i):
            for owner in range(devices):
                slot = jnp.bitwise_xor(owner, me)
                slot = (slot & 1) * (devices // 2) + (slot >> 1)
                for g in range(group):
                    at = g * box + owner * owned
                    coefficients[at : at + owned] = slots_ref[slot, i * group + g]
            sorted_rows = [
                coefficients[pl.ds(g * box + r, box // 4, stride=4)]
                for g in range(group)
                for r in range(4)
            ]
            high, low = split(jnp.concatenate(sorted_rows, 0))
            turned = dot(jnp.concatenate([high, low, high], 1), x_back_ref[...])
            high, low = split(turned)
            for g in range(group):
                even = slice(g * box, g * box + box // 2)
                odd = slice(g * box + box // 2, (g + 1) * box)
                at = slice(g * rows, (g + 1) * rows)
                lines[i, at, :box] = jnp.concatenate([high[even], low[even]], 0).T
                lines[i, at, box : 2 * box] = high[g * box : (g + 1) * box].T
                lines[i, at, 2 * box :] = jnp.concatenate([high[odd], low[odd]], 0).T

        def along_y(i):
            slot = i % stages
            mine = pl.ds(i * group, group)
            for n in range(0, ny // 2, tile):
                at = slice(n, n + tile)
                even = dot(lines[i, :, : 2 * box], back_ref[0, :, at]).reshape(group, rows, tile)
                odd = dot(lines[i, :, box:], back_ref[1, :, at]).reshape(group, rows, tile)
                for start, change in ((n, even + odd), (n + ny // 2, even - odd)):
                    at = pl.ds(start, tile)
                    stage[slot, :, :, at] = held_ref[mine, :, at] + change
                    pltpu.make_async_copy(
                        stage.at[slot, :, :, at], out_ref.at[mine, :, at], sent.at[slot]
                    ).start()

        along_x(0)

        @pl.loop(0, steps)
        def _(i):
            @pl.when(i >= stages)
            def _():
                copy(i - stages).wait()

            along_y(i)
            along_x(jnp.minimum(i + 1, steps - 1))

        for i in range(steps - stages, steps):
            copy(i).wait()

    vmem = pl.BlockSpec(memory_space=pltpu.VMEM)
    hbm = pl.BlockSpec(memory_space=pl.ANY)
    in_specs = [pl.BlockSpec(memory_space=pltpu.SMEM), vmem, vmem, vmem, vmem]
    near = [pltpu.with_memory_space_constraint(a, pltpu.VMEM) for a in (held, slots, back, x_back)]
    return pl.pallas_call(
        kernel,
        name="inverse",
        out_shape=jax.ShapeDtypeStruct(held.shape, F32),
        in_specs=in_specs,
        out_specs=hbm,
        scratch_shapes=[
            pltpu.VMEM((group * box, box), F32),
            pltpu.VMEM((steps, group * rows, 3 * box), BF16),
            pltpu.VMEM((stages, group, rows, ny), F32),
            pltpu.SemaphoreType.DMA((stages,)),
        ],
        compiler_params=pltpu.CompilerParams(vmem_limit_bytes=28 << 20),
        cost_estimate=pl.CostEstimate(
            flops=2 * 3 * count * rows * ny * box,
            bytes_accessed=4 * count * rows * ny,
            transcendentals=0,
        ),
    )(place, *near)


def exchange(value, bit, devices):
    return lax.ppermute(value, "row", [(i, i ^ bit) for i in range(devices)])


def reduce_to_owner(keep, send, devices):
    rest = range(1, devices // 4)
    total = keep + exchange(send, 1, devices)
    pairs = total.reshape(devices // 4, 2, *total.shape[1:])
    one = exchange(pairs[1:, 1], 2, devices)
    far = pairs[1:, 0] + one
    others = [exchange(far[k - 1], 4 * k, devices) for k in rest]
    one = exchange(pairs[0, 1], 2, devices)
    return sum(others, pairs[0, 0] + one)


def gather_from_owners(own, devices):
    rest = range(1, devices // 4)
    last = exchange(own, 4, devices)
    others = [last] + [exchange(own, 4 * k, devices) for k in rest[1:]]
    across = exchange(own, 2, devices)
    others = jnp.stack(others)
    near = jnp.concatenate([own[None], others], 0)
    far = jnp.concatenate([across[None], exchange(others, 2, devices)], 0)

    def pair(a, b):
        return jnp.stack([a, b], 1).reshape(devices // 2, *own.shape)

    return pair(near, far), pair(exchange(near, 1, devices), exchange(far, 1, devices))


def prepare(host, weights, cut_x, cut_y, table_index, place, table, table_x, rows, nx, ny):
    owned, _, variables, levels, box = host.shape
    half_box = box // 2
    fields = variables * levels
    signed = np.arange(box)[:, None] - half_box
    target = np.arange(box)[None, :]
    match = (np.abs(signed) == target // 2) & (np.abs(signed) < half_box)
    to_cos = np.where(match & (target % 2 == 0), 1.0, 0.0)
    to_sin = np.where(match & (target % 2 == 1), -np.sign(signed), 0.0)
    fold = jnp.asarray(np.concatenate([to_cos, to_sin], 0).astype(BF16))

    def kernel(
        place_ref, weights_ref, cut_x_ref, cut_y_ref, index_ref, host_ref, fold_ref, table_ref,
        far_x_ref, wanted_ref, factor_ref, back_ref, x_back_ref, below_ref,
        rows_ref, table_x_ref, turned_ref, arrived,
    ):
        fetch = pltpu.make_async_copy(
            far_x_ref.at[pl.ds(place_ref[0] * rows, rows)], table_x_ref, arrived.at[0]
        )
        fetch.start()
        most = cut_x_ref[0]
        for l in range(levels):
            most = jnp.maximum(most, jnp.maximum(cut_x_ref[l], cut_y_ref[l]))
        below_ref[0] = (most < half_box).astype(jnp.int32)
        j = lax.broadcasted_iota(jnp.int32, (owned, box), 0)
        a = lax.broadcasted_iota(jnp.int32, (owned, box), 1)
        b = place_ref[0] * owned + j
        even = j % 2 == 0
        wave_x = jnp.where(a == 1, half_box, a >> 1)
        wave_y = jnp.where(b == 1, half_box, b >> 1)
        twice = jnp.where(a == 0, 1.0, 2.0) * jnp.where(b == 0, 1.0, 2.0) / (nx * ny)

        def partner(value):
            return jnp.where(even, jnp.roll(value, -1, 0), jnp.roll(value, 1, 0))

        for v in range(variables):
            for l in range(levels):
                at = v * levels + l
                real = jnp.where(b == 1, 0.0, host_ref[:, 0, v, l, :])
                imag = jnp.where(b == 1, 0.0, host_ref[:, 1, v, l, :])
                real_pair, imag_pair = partner(real), partner(imag)
                own = slice(at * owned, (at + 1) * owned)
                rows_ref[own, :box] = jnp.where(even, real + real_pair, imag - imag_pair)
                rows_ref[own, box:] = jnp.where(even, imag + imag_pair, real_pair - real)
        rest = rows_ref[...]
        folded = jnp.zeros((fields * owned, box), F32)
        for _ in range(3):
            part = rest.astype(BF16)
            rest = rest - part.astype(F32)
            folded = folded + dot(part, fold_ref[...])
        for v in range(variables):
            for l in range(levels):
                at = v * levels + l
                inside = (wave_x <= cut_x_ref[l]) & (wave_y <= cut_y_ref[l])
                scale = jnp.where(inside, weights_ref[v, index_ref[l]], 0.0)
                wanted_ref[at] = scale * folded[at * owned : (at + 1) * owned]
                factor_ref[at] = scale * twice
        fetch.wait()
        high = table_x_ref[:, :box].T
        x_back_ref[:box] = high
        x_back_ref[box : 2 * box] = high
        x_back_ref[2 * box :] = table_x_ref[:, box:].T
        quarter, half = box // 4, box // 2
        none = jnp.zeros((half, ny // 2), BF16)
        back_ref[0, 3 * half :] = none
        back_ref[1, :half] = none
        for c in range(0, ny // 2, box):
            at = slice(c, c + box)
            for part in range(2):
                turned_ref[...] = table_ref[at, part * box : (part + 1) * box].astype(F32).T
                rows_of = [turned_ref[pl.ds(r, quarter, stride=4)] for r in range(4)]
                even = jnp.concatenate(rows_of[:2], 0).astype(BF16)
                odd = jnp.concatenate(rows_of[2:], 0).astype(BF16)
                if part == 0:
                    back_ref[0, :half, at] = even
                    back_ref[0, half : 2 * half, at] = even
                    back_ref[1, 2 * half : 3 * half, at] = odd
                    back_ref[1, 3 * half :, at] = odd
                else:
                    back_ref[0, 2 * half : 3 * half, at] = even
                    back_ref[1, half : 2 * half, at] = odd

    smem = pl.BlockSpec(memory_space=pltpu.SMEM)
    vmem = pl.BlockSpec(memory_space=pltpu.VMEM)
    far_x = pltpu.with_memory_space_constraint(table_x, pltpu.HBM)
    flat = jax.ShapeDtypeStruct((fields, owned, box), F32)
    return pl.pallas_call(
        kernel,
        name="prepare",
        out_shape=(
            flat,
            flat,
            pltpu.VMEM((2, 2 * box, ny // 2), BF16),
            pltpu.VMEM((3 * box, rows), BF16),
            jax.ShapeDtypeStruct((1,), jnp.int32),
        ),
        in_specs=[smem] * 5 + [vmem] * 3 + [pl.BlockSpec(memory_space=pltpu.HBM)],
        out_specs=(vmem, vmem, vmem, vmem, smem),
        scratch_shapes=[
            pltpu.VMEM((fields * owned, 2 * box), F32),
            pltpu.VMEM((rows, 2 * box), BF16),
            pltpu.VMEM((box, box), F32),
            pltpu.SemaphoreType.DMA((1,)),
        ],
        compiler_params=pltpu.CompilerParams(vmem_limit_bytes=8 << 20),
    )(place, weights.T, cut_x, cut_y, table_index, host, fold, table, far_x)


def below_edge(field, host, weights, cut_x, cut_y, table_index):
    variables, levels, rows, ny = field.shape
    devices = lax.axis_size("row")
    place = lax.axis_index("row")
    nx = rows * devices
    box = host.shape[4]
    fields = variables * levels
    flat = field.reshape(fields, rows, ny)
    me = place.astype(jnp.int32).reshape(1)
    high, low = basis(ny, box)
    table = jnp.asarray(np.concatenate([high, low], 1))
    if nx == ny:
        table_x = table
    else:
        table_x = jnp.asarray(np.concatenate(basis(nx, box), 1))
    wanted, factor, back, x_back, below = prepare(
        host, weights, cut_x, cut_y, table_index, me, table, table_x, rows, nx, ny
    )
    slots, held = forward(flat, table, table_x, me, devices)
    total = reduce_to_owner(slots[: devices // 2], slots[devices // 2 :], devices)
    slots = jnp.concatenate(gather_from_owners(wanted - factor * total, devices), 0)
    out = inverse(held, slots, back, x_back, me)
    return out.reshape(field.shape), below[0]


def shards(field, host, weights, cut_x, cut_y, table_index):
    args = (field, host, weights, cut_x, cut_y, table_index)
    branches = (lambda out, *rest: any_cutoff(*rest), lambda out, *rest: out)
    usual, below = below_edge(*args)
    return lax.switch(below, branches, usual, *args)


def solution(mesh):
    return jax.shard_map(
        shards,
        mesh=mesh,
        in_specs=(
            P("member", None, "row", None),
            P("row", None, "member", None, None),
            P(),
            P(),
            P(),
            P(),
        ),
        out_specs=P("member", None, "row", None),
        check_vma=False,
    )
```
